768 devices in a mesh: lon: 16 (over x, z_hi), lat: 48 (over z_lo, y, core).
Axes of the slice: x: 4, y: 8, z: 12 (z_hi: 4, z_lo: 3; z = z_hi * 3 + z_lo), core: 2. Of those that a mesh axis runs over, the one named last changes fastest.
Arguments:
- spectrum: float32 [128, 3072, 648], P('lon', 'lat'), may hold values from 0.01 to 1
- sea_mask: int32 [128, 3072], P('lon', 'lat'), may hold values from 0 to 1, as said below
- ice_flags: int32 [128, 3072], P('lon', 'lat'), may hold values 0 or 1
- wind_forcing: float32 [128, 3072], P('lon', 'lat'), may hold values from 0.1 to 1.5
- group_speed: float32 [18], replicated, may hold values from 0.3 to 1
- coupling: bfloat16 [648, 648], replicated, may hold values from -0.25 to 0.25
Outputs:
- field: float32 [128, 3072, 648], P('lon', 'lat')
The draws below stay inside these ranges and needn't reach their ends.
Inputs may be any that keep to these rules, and one draw needn't show every extreme that they name: `sea_mask`: each device's block of 8 x 64 cells holds at most 384 sea cells and at least 128; in every draw some block holds exactly 384.
All inputs are finite; a program needn't handle non-finite values. No bound on the sum of `ice_flags` on one device may be relied on, other than what follows from the above.
Results may differ from the reference program's by a relative error of at most 0.00079.
Values sent between devices are 32-bit elements; how exact they have to be, the bound alone decides.
A program may use at most 32 MiB of HBM per device.

```python
import math
import jax
import jax.numpy as jnp

DIRS = 36
FREQS = 18
BINS = 648
CX = 8
CY = 64
SEA_DEV = 384
STEPS = 4
NX = 128
NY = 3072


def draw_sea_mask(key, part):
    blocks_x = NX // CX
    blocks_y = NY // CY
    cells = CX * CY
    blocks = blocks_x * blocks_y
    key_count, key_pick, key_order = jax.random.split(jax.random.fold_in(key, 11), 3)
    counts = jax.random.randint(key_count, (blocks,), SEA_DEV // 3, SEA_DEV + 1)
    chosen = jax.random.randint(key_pick, (), 0, blocks)
    counts = counts.at[chosen].set(SEA_DEV)
    scores = jax.random.randint(key_order, (blocks, cells), 0, 2 ** 20) * cells + jnp.arange(cells, dtype=jnp.int32)[None, :]
    order = jnp.argsort(scores, axis=1, stable=True)
    ranks = jnp.argsort(order, axis=1, stable=True)
    flags = (ranks < counts[:, None]).astype(jnp.int32)
    flags = flags.reshape(blocks_x, blocks_y, CX, CY).transpose(0, 2, 1, 3)
    return flags.reshape(NX, NY)


def set_ends(array, key, low, largest):
    dims = array.shape
    index_at = [jax.random.randint(jax.random.fold_in(key, axis), (), 0, dims[axis]) for axis in range(len(dims))]
    array = array.at[tuple(index_at)].set(low)
    longest = dims.index(max(dims))
    index_at[longest] = (index_at[longest] + 1) % dims[longest]
    return array.at[tuple(index_at)].set(largest)


def levels(key, shape, cuts, least, largest):
    gain = 1.0
    for dim, parts in cuts:
        heights = jax.random.uniform(jax.random.fold_in(jax.random.fold_in(key, 6), dim), (parts,), jnp.float32, least / len(cuts), largest / len(cuts))
        gain = gain * jnp.repeat(jnp.exp(heights), shape[dim] // parts).reshape((-1,) + (1,) * (len(shape) - 1 - dim))
    return gain


def noise(stream_key, extent, scale, limit, kind=jnp.bfloat16):
    return jnp.clip(scale * jax.random.normal(stream_key, extent, jnp.float32), -limit, limit).astype(kind)


def setup_inputs(seed: int = 0) -> dict:
    arg_keys = jax.random.split(jax.random.key(seed), 7)
    spectrum = jnp.clip(jnp.exp(math.log(1.0) - 4.6051702 * jax.random.uniform(arg_keys[0], (NX, NY, BINS), jnp.float32) ** levels(arg_keys[0], (NX, NY, BINS), ((0, 16), (1, 48)), -0.2, 0.2)), 0.01, 1.0)
    sea_mask = draw_sea_mask(jax.random.fold_in(arg_keys[6], 71), 0)
    ice_flags = set_ends((jax.random.randint(arg_keys[2], (NX, NY), 0, 4) < 1).astype(jnp.int32), jax.random.fold_in(arg_keys[2], 1), 0, 1)
    wind_forcing = jnp.clip(jnp.exp(math.log(1.5) - 2.7080502 * jax.random.uniform(arg_keys[3], (NX, NY), jnp.float32) ** levels(arg_keys[3], (NX, NY), ((0, 16), (1, 48)), -0.2, 0.2)), 0.1, 1.5)
    group_speed = jnp.clip(jax.random.uniform(arg_keys[4], (FREQS,), jnp.float32, 0.3, 1.0), 0.3, 1.0)
    coupling = noise(arg_keys[5], (BINS, BINS), BINS ** -0.5, 0.25)
    return {"spectrum": spectrum, "sea_mask": sea_mask, "ice_flags": ice_flags, "wind_forcing": wind_forcing, "group_speed": group_speed, "coupling": coupling}


time_step = 0.2
dissipation = 0.5


def speed_tables(rows, total_rows, group_speed, dirs):
    theta = (jnp.arange(dirs).astype(jnp.float32) + 0.5) * (2.0 * math.pi / dirs)
    latitude = (-60.0 + 120.0 * (rows.astype(jnp.float32) + 0.5) / total_rows) * (math.pi / 180.0)
    scaled = jnp.outer(jnp.cos(theta), group_speed).reshape(-1)
    along_x = (0.225 * scaled)[None, :] / jnp.cos(latitude)[:, None]
    along_y = 0.45 * jnp.outer(jnp.sin(theta), group_speed).reshape(-1)
    return along_x, along_y


def upwind(field, west, east, south, north, along_x, along_y):
    speed_x = along_x[None]
    result = field - jnp.maximum(speed_x, 0.0) * (field - west) - jnp.minimum(speed_x, 0.0) * (east - field)
    return result - jnp.maximum(along_y, 0.0) * (field - south) - jnp.minimum(along_y, 0.0) * (north - field)


def sources(advected, wind_forcing, ice_flags, coupling):
    shape = advected.shape
    energy = jnp.mean(advected, axis=-1, keepdims=True)
    flat = advected.reshape(-1, shape[-1]).astype(jnp.bfloat16)
    transfer = jnp.dot(flat, coupling, preferred_element_type=jnp.float32).reshape(shape)
    forcing = (wind_forcing * (1.0 - ice_flags.astype(jnp.float32)))[..., None]
    return advected + time_step * (forcing * advected + transfer - dissipation * energy * advected)


def reference(spectrum, sea_mask, ice_flags, wind_forcing, group_speed, coupling):
    sea = sea_mask.astype(jnp.float32)[..., None]
    along_x, along_y = speed_tables(jnp.arange(NY), NY, group_speed, DIRS)
    field = spectrum * sea
    for step in range(STEPS):
        west = jnp.roll(field, 1, axis=0)
        east = jnp.roll(field, -1, axis=0)
        edge = jnp.zeros_like(field[:, :1])
        south = jnp.concatenate([edge, field[:, :-1]], axis=1)
        north = jnp.concatenate([field[:, 1:], edge], axis=1)
        advected = upwind(field, west, east, south, north, along_x, along_y)
        field = sources(advected, wind_forcing, ice_flags, coupling) * sea
    return field
```

```python
import functools
import math

import jax
import jax.numpy as jnp
import numpy as np
from jax import lax
from jax.experimental import pallas as pl
from jax.experimental.pallas import tpu as pltpu
from jax.sharding import PartitionSpec as P

DIRS = 36
STEPS = 4
TIME_STEP = 0.2
DISSIPATION = 0.5
LANES = 128
TILES = 6
WIDE = TILES * LANES
CHUNK = 16
PAD = 8
ORDER = (0, 3, 1, 2)
MESH = pl.DeviceIdType.MESH


def direction_rows(freqs):
    theta = ((np.arange(DIRS, dtype=np.float32) + np.float32(0.5)) * np.float32(2.0 * math.pi / DIRS))
    rows = np.zeros((8, WIDE), np.float32)
    bins = DIRS * freqs
    rows[0, :bins] = np.repeat(np.abs(np.cos(theta)), freqs)
    rows[1, :bins] = np.repeat(np.abs(np.sin(theta)), freqs)
    rows[2, :bins] = np.tile(np.arange(freqs), DIRS)
    rows[2, bins:] = -1.0
    return rows


def kernel(
    sizes,
    spectrum, sea, ice, wind, speed, coupling, rows_in,
    out,
    raw, field, sea_v, ice_v, wind_v, speed_s, couple_raw, couple, rows_v,
    keep, along_x, along_y, share, gain, moved, rounded,
    send, recv,
    in_sem, lon_send, lon_recv, lat_send, lat_recv,
):
    n_lon, n_lat, bins, freqs = sizes
    cx, cy = spectrum.shape[0], spectrum.shape[1]
    chunks = cy // CHUNK
    lon, lat = lax.axis_index("lon"), lax.axis_index("lat")
    east, west = lax.rem(lon + 1, n_lon), lax.rem(lon + n_lon - 1, n_lon)
    has_south, has_north = lat > 0, lat < n_lat - 1
    lane = lax.broadcasted_iota(jnp.int32, (CHUNK, LANES), 1)

    columns = (0, cx - 1) + tuple(range(1, cx - 1))
    column_in = {i: pltpu.make_async_copy(spectrum.at[i], raw.at[i], in_sem.at[i]) for i in columns}
    small = [
        pltpu.make_async_copy(src, dst, in_sem.at[cx + n])
        for n, (src, dst) in enumerate(
            [(sea, sea_v), (ice, ice_v), (wind, wind_v), (speed, speed_s), (rows_in, rows_v)]
        )
    ]
    couple_in = pltpu.make_async_copy(coupling, couple_raw, in_sem.at[cx + 5])
    for copy in small:
        copy.start()
    for i in columns:
        column_in[i].start()
    couple_in.start()

    zero = jnp.zeros((PAD, WIDE), jnp.float32)
    for par in range(2):
        for i in range(cx):
            field[par, i, 0:PAD, :] = zero
            field[par, i, PAD + cy : PAD + cy + PAD, :] = zero

    barrier = pltpu.get_barrier_semaphore()
    pl.semaphore_signal(barrier, inc=1, device_id={"lon": east}, device_id_type=MESH)
    pl.semaphore_signal(barrier, inc=1, device_id={"lon": west}, device_id_type=MESH)

    @pl.when(has_south)
    def _():
        pl.semaphore_signal(barrier, inc=1, device_id={"lat": lat - 1}, device_id_type=MESH)

    @pl.when(has_north)
    def _():
        pl.semaphore_signal(barrier, inc=1, device_id={"lat": lat + 1}, device_id_type=MESH)

    for copy in small:
        copy.wait()
    speed_row = jnp.zeros((1, WIDE), jnp.float32)
    which = rows_v[2:3, :]
    for f in range(freqs):
        speed_row = jnp.where(which == f, speed_s[f], speed_row)
    scaled_x = 0.225 * (rows_v[0:1, :] * speed_row)
    scaled_y = 0.45 * (rows_v[1:2, :] * speed_row)
    row = (lat * cy + lax.broadcasted_iota(jnp.int32, (cy, LANES), 0)).astype(jnp.float32)
    phi = (-60.0 + 120.0 * (row + 0.5) / (cy * n_lat)) * (math.pi / 180.0)
    square = phi * phi
    cosine = jnp.full((cy, LANES), 1.0 / math.factorial(16), jnp.float32)
    for term in range(7, -1, -1):
        cosine = cosine * square + (-1.0) ** term / math.factorial(2 * term)
    inverse = 1.0 / cosine
    along_y[...] = jnp.broadcast_to(scaled_y, (8, WIDE))
    for k in range(TILES):
        cut = slice(k * LANES, (k + 1) * LANES)
        speed_x = inverse * scaled_x[:, cut]
        along_x[:, cut] = speed_x
        keep[:, cut] = 1.0 - speed_x - scaled_y[:, cut]

    sea_f = sea_v[...].astype(jnp.float32)
    forcing = wind_v[...] * (1.0 - ice_v[...].astype(jnp.float32))
    gain_t = jnp.transpose(sea_f * (1.0 + TIME_STEP * forcing))
    sea_t = jnp.transpose(sea_f)
    for i in range(cx):
        share[i] = TIME_STEP * jnp.broadcast_to(sea_t[:, i : i + 1], (cy, LANES))
        gain[i] = jnp.broadcast_to(gain_t[:, i : i + 1], (cy, LANES))

    def load_column(i):
        sea_i = jnp.broadcast_to(sea_t[:, i : i + 1], (cy, LANES))
        for k in range(TILES):
            cut = slice(k * LANES, (k + 1) * LANES)
            if (k + 1) * LANES <= bins:
                field[0, i, PAD : PAD + cy, cut] = raw[i, :, cut] * sea_i
            else:
                tail = bins - k * LANES
                last = raw[i, :, k * LANES : bins] * sea_i[:, :tail]
                field[0, i, PAD : PAD + cy, cut] = jnp.concatenate(
                    [last, jnp.zeros((cy, LANES - tail), jnp.float32)], axis=1
                )

    def lon_copy(side, par, c):
        return pltpu.make_async_remote_copy(
            src_ref=send.at[side, par, c],
            dst_ref=recv.at[side, par, c],
            send_sem=lon_send.at[side, par, c],
            recv_sem=lon_recv.at[side, par, c],
            device_id={"lon": west if side else east},
            device_id_type=MESH,
        )

    def lat_copy(side, par):
        if side == 0:
            src = field.at[par, :, PAD + cy - 1 : PAD + cy, 0 : 3 * LANES]
            dst = field.at[par, :, PAD - 1 : PAD, 0 : 3 * LANES]
        else:
            src = field.at[par, :, PAD : PAD + 1, 2 * LANES : WIDE]
            dst = field.at[par, :, PAD + cy : PAD + cy + 1, 2 * LANES : WIDE]
        return pltpu.make_async_remote_copy(
            src_ref=src,
            dst_ref=dst,
            send_sem=lat_send.at[side, par],
            recv_sem=lat_recv.at[side, par],
            device_id={"lat": lat - 1 if side else lat + 1},
            device_id_type=MESH,
        )

    def lat_start(par):
        @pl.when(has_north)
        def _():
            lat_copy(0, par).start()

        @pl.when(has_south)
        def _():
            lat_copy(1, par).start()

    def lat_wait_send(par):
        @pl.when(has_north)
        def _():
            lat_copy(0, par).wait_send()

        @pl.when(has_south)
        def _():
            lat_copy(1, par).wait_send()

    def lat_wait_recv(par):
        @pl.when(has_south)
        def _():
            lat_copy(0, par).wait_recv()

        @pl.when(has_north)
        def _():
            lat_copy(1, par).wait_recv()

    def pack_east(par, c, t):
        send[0, par, c, 0] = t[0]
        send[0, par, c, 1] = t[4]
        tail = pltpu.roll(t[5], 34, 1)
        send[0, par, c, 2] = jnp.where(lane < 34, t[1], jnp.where(lane < 102, tail, t[3]))

    def pack_west(par, c, t):
        send[1, par, c, 0] = t[2]
        send[1, par, c, 1] = jnp.where(lane < 34, t[3], t[1])
        send[1, par, c, 2] = t[3]

    def tile(par, i, r0, k):
        return field[par, i, PAD + r0 : PAD + r0 + CHUNK, k * LANES : (k + 1) * LANES]

    def advect(par, i, c):
        r0 = c * CHUNK
        if i == 0:
            a, b, m = recv[0, par, c, 0], recv[0, par, c, 1], recv[0, par, c, 2]
            from_west = {0: a, 1: m, 3: m, 4: b, 5: pltpu.roll(m, LANES - 34, 1)}
        else:
            from_west = {k: tile(par, i - 1, r0, k) for k in (0, 1, 3, 4, 5)}
        if i == cx - 1:
            a, b, m = recv[1, par, c, 0], recv[1, par, c, 1], recv[1, par, c, 2]
            from_east = {1: b, 2: a, 3: jnp.where(lane < 34, b, m)}
        else:
            from_east = {k: tile(par, i + 1, r0, k) for k in (1, 2, 3)}
        up_x = [
            from_west[0],
            jnp.where(lane < 34, from_west[1], from_east[1]),
            from_east[2],
            jnp.where(lane < 102, from_east[3], from_west[3]),
            from_west[4],
            from_west[5],
        ]
        out_tiles = []
        for k in range(TILES):
            rows = slice(r0, r0 + CHUNK)
            cut = slice(k * LANES, (k + 1) * LANES)
            south = tile(par, i, r0 - 1, k) if k <= 2 else None
            north = tile(par, i, r0 + 1, k) if k >= 2 else None
            up_y = south if north is None else north if south is None else jnp.where(lane < 68, south, north)
            speed_y = jnp.concatenate([along_y[:, cut]] * (CHUNK // 8), axis=0)
            out_tiles.append(
                tile(par, i, r0, k) * keep[rows, cut] + along_x[rows, cut] * up_x[k] + speed_y * up_y
            )
        return out_tiles

    def cell_gain(i, c, t):
        rows = slice(c * CHUNK, (c + 1) * CHUNK)
        total = jnp.sum((t[0] + t[1]) + (t[2] + t[3]) + (t[4] + t[5]), axis=1, keepdims=True)
        return gain[i, rows, :] - share[i, rows, :] * (total * (DISSIPATION / bins))

    def put(par, i, c, tiles, last):
        r0 = c * CHUNK
        for k in range(TILES):
            if not last:
                field[par, i, PAD + r0 : PAD + r0 + CHUNK, k * LANES : (k + 1) * LANES] = tiles[k]
            elif (k + 1) * LANES <= bins:
                out[i, r0 : r0 + CHUNK, k * LANES : (k + 1) * LANES] = tiles[k]
            else:
                out[i, r0 : r0 + CHUNK, k * LANES : bins] = tiles[k][:, : bins - k * LANES]

    def cells(par, blocks, last):
        gains = []
        for n, (i, c) in enumerate(blocks):
            t = advect(par, i, c)
            gains.append(cell_gain(i, c, t))
            for k in range(TILES):
                cut = slice(k * LANES, (k + 1) * LANES)
                moved[n * CHUNK : (n + 1) * CHUNK, cut] = t[k]
                rounded[n * CHUNK : (n + 1) * CHUNK, cut] = t[k].astype(jnp.bfloat16)
        height = len(blocks) * CHUNK
        transfer = jnp.dot(rounded[0:height, :], couple[...], preferred_element_type=jnp.float32)
        results = []
        for n, (i, c) in enumerate(blocks):
            part = share[i, c * CHUNK : (c + 1) * CHUNK, :]
            tiles = []
            for k in range(TILES):
                cut = slice(k * LANES, (k + 1) * LANES)
                rows = slice(n * CHUNK, (n + 1) * CHUNK)
                tiles.append(moved[rows, cut] * gains[n] + transfer[rows, cut] * part)
            put(1 - par, i, c, tiles, last)
            results.append(tiles)
        return results

    def step_body(n, last):
        par = lax.rem(n, 2)
        nxt = 1 - par
        if not last:
            @pl.when(n >= 1)
            def _():
                lat_wait_send(nxt)

        lat_wait_recv(par)
        for place, c in enumerate(ORDER):
            lon_copy(0, par, c).wait_recv()
            lon_copy(1, par, c).wait_recv()
            first, final = cells(par, [(0, c), (cx - 1, c)], last)
            if not last:
                @pl.when(n >= 1)
                def _():
                    lon_copy(0, nxt, c).wait_send()
                    lon_copy(1, nxt, c).wait_send()

                pack_east(nxt, c, final)
                pack_west(nxt, c, first)
                lon_copy(0, nxt, c).start()
                lon_copy(1, nxt, c).start()
            if place % 2 == 1:
                pair = (ORDER[place - 1], c)
                cells(par, [(i, b) for b in pair for i in range(1, cx - 1)], last)
                if place == 1 and not last:
                    lat_start(nxt)

    for i in columns[:2]:
        column_in[i].wait()
        load_column(i)
    for c in ORDER:
        pack_east(0, c, [tile(0, cx - 1, c * CHUNK, k) for k in range(TILES)])
        pack_west(0, c, [tile(0, 0, c * CHUNK, k) for k in range(TILES)])
    peers = 2 + jnp.minimum(lat, 1) + jnp.minimum(n_lat - 1 - lat, 1)
    pl.semaphore_wait(barrier, peers)

    for c in ORDER:
        lon_copy(0, 0, c).start()
        lon_copy(1, 0, c).start()
    for i in columns[2:]:
        column_in[i].wait()
        load_column(i)
    lat_start(0)
    couple_in.wait()
    couple[...] = jnp.zeros(couple.shape, couple.dtype)
    couple[0:bins, 0:bins] = couple_raw[...]

    def loop(n, carry):
        step_body(n, False)
        return carry

    lax.fori_loop(0, STEPS - 1, loop, 0)
    step_body(STEPS - 1, True)
    for par in range(2):
        lat_wait_send(par)
        for c in ORDER:
            lon_copy(0, par, c).wait_send()
            lon_copy(1, par, c).wait_send()


def on_device(n_lon, n_lat, spectrum, sea_mask, ice_flags, wind_forcing, group_speed, coupling):
    cx, cy, bins = spectrum.shape
    freqs = group_speed.shape[0]
    chunks = cy // CHUNK
    f32 = jnp.float32
    dma = pltpu.SemaphoreType.DMA
    scratch = [
        pltpu.VMEM((cx, cy, bins), f32),
        pltpu.VMEM((2, cx, cy + 2 * PAD, WIDE), f32),
        pltpu.VMEM((cx, cy), jnp.int32),
        pltpu.VMEM((cx, cy), jnp.int32),
        pltpu.VMEM((cx, cy), f32),
        pltpu.SMEM((freqs,), f32),
        pltpu.VMEM((bins, bins), jnp.bfloat16),
        pltpu.VMEM((WIDE, WIDE), jnp.bfloat16),
        pltpu.VMEM((8, WIDE), f32),
        pltpu.VMEM((cy, WIDE), f32),
        pltpu.VMEM((cy, WIDE), f32),
        pltpu.VMEM((8, WIDE), f32),
        pltpu.VMEM((cx, cy, LANES), f32),
        pltpu.VMEM((cx, cy, LANES), f32),
        pltpu.VMEM((2 * (cx - 2) * CHUNK, WIDE), f32),
        pltpu.VMEM((2 * (cx - 2) * CHUNK, WIDE), jnp.bfloat16),
        pltpu.VMEM((2, 2, chunks, 3, CHUNK, LANES), f32),
        pltpu.VMEM((2, 2, chunks, 3, CHUNK, LANES), f32),
        dma((cx + 6,)),
        dma((2, 2, chunks)),
        dma((2, 2, chunks)),
        dma((2, 2)),
        dma((2, 2)),
    ]
    anywhere = pl.BlockSpec(memory_space=pl.ANY)
    return pl.pallas_call(
        functools.partial(kernel, (n_lon, n_lat, bins, freqs)),
        out_shape=jax.ShapeDtypeStruct((cx, cy, bins), f32),
        in_specs=[anywhere] * 7,
        out_specs=pl.BlockSpec(memory_space=pltpu.VMEM),
        scratch_shapes=scratch,
        compiler_params=pltpu.CompilerParams(
            collective_id=0, has_side_effects=True, vmem_limit_bytes=63000 * 1024
        ),
    )(spectrum, sea_mask, ice_flags, wind_forcing, group_speed, coupling, jnp.asarray(direction_rows(freqs)))


def solution(mesh):
    placed = (P("lon", "lat", None), P("lon", "lat"), P("lon", "lat"), P("lon", "lat"), P(), P())
    return jax.shard_map(
        functools.partial(on_device, mesh.shape["lon"], mesh.shape["lat"]),
        mesh=mesh, in_specs=placed, out_specs=P("lon", "lat", None), check_vma=False,
    )
```

```python
import functools
import math

import jax
import jax.numpy as jnp
import numpy as np
from jax import lax
from jax.experimental import pallas as pl
from jax.experimental.pallas import tpu as pltpu
from jax.sharding import PartitionSpec as P

DIRS = 36
STEPS = 4
TIME_STEP = 0.2
DISSIPATION = 0.5
LANES = 128
TILES = 6
WIDE = TILES * LANES
CHUNK = 16
WIRE = 2 * CHUNK + 9
DEPTH = 2
PAD = 8
ORDER = (0, 3, 1, 2)
MESH = pl.DeviceIdType.MESH


def direction_rows(freqs):
    theta = ((np.arange(DIRS, dtype=np.float32) + np.float32(0.5)) * np.float32(2.0 * math.pi / DIRS))
    rows = np.zeros((8, WIDE), np.float32)
    bins = DIRS * freqs
    rows[0, :bins] = np.repeat(np.abs(np.cos(theta)), freqs)
    rows[1, :bins] = np.repeat(np.abs(np.sin(theta)), freqs)
    rows[2, :bins] = np.tile(np.arange(freqs), DIRS)
    rows[2, bins:] = -1.0
    return rows


def kernel(
    sizes,
    spectrum, sea, ice, wind, speed, coupling, rows_in,
    out,
    raw, field, sea_v, ice_v, wind_v, speed_s, couple_raw, couple, rows_v,
    keep, along_x, along_y, share, gain, moved, rounded,
    send, recv,
    in_sem, lon_send, lon_recv, lat_send, lat_recv,
):
    n_lon, n_lat, bins, freqs = sizes
    cx, cy = spectrum.shape[0], spectrum.shape[1]
    chunks = cy // CHUNK
    lon, lat = lax.axis_index("lon"), lax.axis_index("lat")
    east, west = lax.rem(lon + 1, n_lon), lax.rem(lon + n_lon - 1, n_lon)
    has_south, has_north = lat > 0, lat < n_lat - 1
    lane = lax.broadcasted_iota(jnp.int32, (CHUNK, LANES), 1)
    lane8, sub8 = lane[0:8], lax.broadcasted_iota(jnp.int32, (8, LANES), 0)

    barrier = pltpu.get_barrier_semaphore()
    pl.semaphore_signal(barrier, inc=1, device_id={"lon": east}, device_id_type=MESH)
    pl.semaphore_signal(barrier, inc=1, device_id={"lon": west}, device_id_type=MESH)

    @pl.when(has_south)
    def _():
        pl.semaphore_signal(barrier, inc=1, device_id={"lat": lat - 1}, device_id_type=MESH)

    @pl.when(has_north)
    def _():
        pl.semaphore_signal(barrier, inc=1, device_id={"lat": lat + 1}, device_id_type=MESH)

    columns = (0, cx - 1) + tuple(range(1, cx - 1))
    column_in = {i: pltpu.make_async_copy(spectrum.at[i], raw.at[i], in_sem.at[i]) for i in columns}
    sea_in, *small = [
        pltpu.make_async_copy(src, dst, in_sem.at[cx + n])
        for n, (src, dst) in enumerate(
            [(sea, sea_v), (ice, ice_v), (wind, wind_v), (speed, speed_s), (rows_in, rows_v)]
        )
    ]
    couple_in = pltpu.make_async_copy(coupling, couple_raw, in_sem.at[cx + 5])
    sea_in.start()
    for i in columns[:2]:
        column_in[i].start()
    for copy in small:
        copy.start()
    for i in columns[2:]:
        column_in[i].start()
    couple_in.start()

    sea_in.wait()
    sea_f = sea_v[...].astype(jnp.float32)
    sea_t = jnp.transpose(sea_f)

    def load_column(i):
        sea_i = jnp.broadcast_to(sea_t[:, i : i + 1], (cy, LANES))
        for k in range(TILES):
            cut = slice(k * LANES, (k + 1) * LANES)
            if (k + 1) * LANES <= bins:
                field[0, i, PAD : PAD + cy, cut] = raw[i, :, cut] * sea_i
            else:
                tail = bins - k * LANES
                last = raw[i, :, k * LANES : bins] * sea_i[:, :tail]
                field[0, i, PAD : PAD + cy, cut] = jnp.concatenate(
                    [last, jnp.zeros((cy, LANES - tail), jnp.float32)], axis=1
                )

    def lon_copy(side, par, c):
        return pltpu.make_async_remote_copy(
            src_ref=send.at[side, par, c],
            dst_ref=recv.at[side, par, c],
            send_sem=lon_send.at[side, par, c],
            recv_sem=lon_recv.at[side, par, c],
            device_id={"lon": west if side else east},
            device_id_type=MESH,
        )

    def lat_copy(side, par):
        if side == 0:
            src = field.at[par, :, PAD + cy - 1 : PAD + cy, 0 : 3 * LANES]
            dst = field.at[par, :, PAD - 1 : PAD, 0 : 3 * LANES]
        else:
            src = field.at[par, :, PAD : PAD + 1, 2 * LANES : WIDE]
            dst = field.at[par, :, PAD + cy : PAD + cy + 1, 2 * LANES : WIDE]
        return pltpu.make_async_remote_copy(
            src_ref=src,
            dst_ref=dst,
            send_sem=lat_send.at[side, par],
            recv_sem=lat_recv.at[side, par],
            device_id={"lat": lat - 1 if side else lat + 1},
            device_id_type=MESH,
        )

    def lat_start(par):
        @pl.when(has_north)
        def _():
            lat_copy(0, par).start()

        @pl.when(has_south)
        def _():
            lat_copy(1, par).start()

    def lat_wait_send(par):
        @pl.when(has_north)
        def _():
            lat_copy(0, par).wait_send()

        @pl.when(has_south)
        def _():
            lat_copy(1, par).wait_send()

    def lat_wait_recv(par):
        @pl.when(has_south)
        def _():
            lat_copy(0, par).wait_recv()

        @pl.when(has_north)
        def _():
            lat_copy(1, par).wait_recv()

    def tables():
        for copy in small:
            copy.wait()
        speed_row = jnp.zeros((1, WIDE), jnp.float32)
        which = rows_v[2:3, :]
        for f in range(freqs):
            speed_row = jnp.where(which == f, speed_s[f], speed_row)
        scaled_x = 0.225 * (rows_v[0:1, :] * speed_row)
        scaled_y = 0.45 * (rows_v[1:2, :] * speed_row)
        row = (lat * cy + lax.broadcasted_iota(jnp.int32, (cy, LANES), 0)).astype(jnp.float32)
        phi = (-60.0 + 120.0 * (row + 0.5) / (cy * n_lat)) * (math.pi / 180.0)
        square = phi * phi
        cosine = jnp.full((cy, LANES), 1.0 / math.factorial(16), jnp.float32)
        for term in range(7, -1, -1):
            cosine = cosine * square + (-1.0) ** term / math.factorial(2 * term)
        inverse = 1.0 / cosine
        along_y[...] = jnp.broadcast_to(scaled_y, (8, WIDE))
        for k in range(TILES):
            cut = slice(k * LANES, (k + 1) * LANES)
            speed_x = inverse * scaled_x[:, cut]
            along_x[:, cut] = speed_x
            keep[:, cut] = 1.0 - speed_x - scaled_y[:, cut]

        forcing = wind_v[...] * (1.0 - ice_v[...].astype(jnp.float32))
        gain_t = jnp.transpose(sea_f * (1.0 + TIME_STEP * forcing))
        for i in range(cx):
            share[i] = TIME_STEP * jnp.broadcast_to(sea_t[:, i : i + 1], (cy, LANES))
            gain[i] = jnp.broadcast_to(gain_t[:, i : i + 1], (cy, LANES))

    def squeeze(side, par, c, first, second, rest):
        send[side, par, c, 0:CHUNK] = first
        send[side, par, c, CHUNK : 2 * CHUNK] = second
        low, high = rest[0:8], rest[8:16]
        send[side, par, c, 2 * CHUNK : 2 * CHUNK + 8] = jnp.where(lane8 < 64, low, pltpu.roll(high, 64, 1))
        line = jnp.zeros((8, LANES), jnp.float32)
        for half, part in enumerate((low, high)):
            part = jnp.where((lane8 >= 64) & (lane8 < 68), part, 0.0)
            for r in range(8):
                spot = 32 * half + 4 * r
                line = line + jnp.where(sub8 == r, pltpu.roll(part, (64 + spot) % LANES, 1), 0.0)
        send[side, par, c, 2 * CHUNK + 8 : 2 * CHUNK + 9] = jnp.sum(line, axis=0, keepdims=True)

    def spread(side, par, c):
        first = recv[side, par, c, 0:CHUNK]
        second = recv[side, par, c, CHUNK : 2 * CHUNK]
        both = recv[side, par, c, 2 * CHUNK : 2 * CHUNK + 8]
        line = jnp.broadcast_to(recv[side, par, c, 2 * CHUNK + 8 : 2 * CHUNK + 9], (8, LANES))
        parts = []
        for half, body in enumerate((both, pltpu.roll(both, 64, 1))):
            tail = line
            for r in range(8):
                spot = 32 * half + 4 * r
                tail = jnp.where(sub8 == r, pltpu.roll(line, (64 - spot) % LANES, 1), tail)
            parts.append(jnp.where(lane8 < 64, body, tail))
        return first, second, jnp.concatenate(parts, axis=0)

    def pack_east(par, c, t):
        rest = jnp.where(lane < 34, t[1], jnp.where(lane < 102, pltpu.roll(t[5], 34, 1), t[3]))
        squeeze(0, par, c, t[0], t[4], pltpu.roll(rest, 26, 1))

    def pack_west(par, c, t):
        squeeze(1, par, c, t[2], jnp.where(lane < 34, t[3], t[1]), pltpu.roll(t[3], LANES - 34, 1))

    def unpack_east(par, c):
        first, second, rest = spread(0, par, c)
        mixed = pltpu.roll(rest, LANES - 26, 1)
        return {0: first, 1: mixed, 3: mixed, 4: second, 5: pltpu.roll(rest, LANES - 60, 1)}

    def unpack_west(par, c):
        first, second, rest = spread(1, par, c)
        return {1: second, 2: first, 3: jnp.where(lane < 34, second, pltpu.roll(rest, 34, 1))}

    def tile(par, i, r0, k):
        return field[par, i, PAD + r0 : PAD + r0 + CHUNK, k * LANES : (k + 1) * LANES]

    def advect(par, i, c):
        r0 = c * CHUNK
        if i == 0:
            from_west = unpack_east(par, c)
        else:
            from_west = {k: tile(par, i - 1, r0, k) for k in (0, 1, 3, 4, 5)}
        if i == cx - 1:
            from_east = unpack_west(par, c)
        else:
            from_east = {k: tile(par, i + 1, r0, k) for k in (1, 2, 3)}
        up_x = [
            from_west[0],
            jnp.where(lane < 34, from_west[1], from_east[1]),
            from_east[2],
            jnp.where(lane < 102, from_east[3], from_west[3]),
            from_west[4],
            from_west[5],
        ]
        out_tiles = []
        for k in range(TILES):
            rows = slice(r0, r0 + CHUNK)
            cut = slice(k * LANES, (k + 1) * LANES)
            south = tile(par, i, r0 - 1, k) if k <= 2 else None
            north = tile(par, i, r0 + 1, k) if k >= 2 else None
            up_y = south if north is None else north if south is None else jnp.where(lane < 68, south, north)
            speed_y = jnp.concatenate([along_y[:, cut]] * (CHUNK // 8), axis=0)
            out_tiles.append(
                tile(par, i, r0, k) * keep[rows, cut] + along_x[rows, cut] * up_x[k] + speed_y * up_y
            )
        return out_tiles

    def cell_gain(i, c, t):
        rows = slice(c * CHUNK, (c + 1) * CHUNK)
        total = jnp.sum((t[0] + t[1]) + (t[2] + t[3]) + (t[4] + t[5]), axis=1, keepdims=True)
        return gain[i, rows, :] - share[i, rows, :] * (total * (DISSIPATION / bins))

    def put(par, i, c, tiles, last):
        r0 = c * CHUNK
        for k in range(TILES):
            if not last:
                field[par, i, PAD + r0 : PAD + r0 + CHUNK, k * LANES : (k + 1) * LANES] = tiles[k]
            elif (k + 1) * LANES <= bins:
                out[i, r0 : r0 + CHUNK, k * LANES : (k + 1) * LANES] = tiles[k]
            else:
                out[i, r0 : r0 + CHUNK, k * LANES : bins] = tiles[k][:, : bins - k * LANES]

    def cells(par, blocks, last):
        gains = []
        for n, (i, c) in enumerate(blocks):
            t = advect(par, i, c)
            gains.append(cell_gain(i, c, t))
            for k in range(TILES):
                cut = slice(k * LANES, (k + 1) * LANES)
                moved[n * CHUNK : (n + 1) * CHUNK, cut] = t[k]
                rounded[n * CHUNK : (n + 1) * CHUNK, cut] = t[k].astype(jnp.bfloat16)
        height = len(blocks) * CHUNK
        transfer = jnp.dot(rounded[0:height, :], couple[...], preferred_element_type=jnp.float32)
        results = []
        for n, (i, c) in enumerate(blocks):
            part = share[i, c * CHUNK : (c + 1) * CHUNK, :]
            tiles = []
            for k in range(TILES):
                cut = slice(k * LANES, (k + 1) * LANES)
                rows = slice(n * CHUNK, (n + 1) * CHUNK)
                tiles.append(moved[rows, cut] * gains[n] + transfer[rows, cut] * part)
            put(1 - par, i, c, tiles, last)
            results.append(tiles)
        return results

    def pace(place, par):
        back = place - DEPTH
        which = par if back >= 0 else 1 - par
        for side in range(2):
            lon_copy(side, which, ORDER[back]).wait_send()

    def inner(par, pair, last):
        cells(par, [(i, b) for b in pair for i in range(1, cx - 1)], last)

    def step_body(n, last):
        par = lax.rem(n, 2)
        nxt = 1 - par
        if not last:
            @pl.when(n >= 1)
            def _():
                lat_wait_send(nxt)

        lat_wait_recv(par)
        if last:
            inner(par, ORDER[0:2], last)
            inner(par, ORDER[2:4], last)
        for place, c in enumerate(ORDER):
            lon_copy(0, par, c).wait_recv()
            lon_copy(1, par, c).wait_recv()
            first, final = cells(par, [(0, c), (cx - 1, c)], last)
            if last:
                continue
            pack_east(nxt, c, final)
            pack_west(nxt, c, first)
            if place % 2 == 1:
                inner(par, ORDER[place - 1 : place + 1], last)
                if place == 1:
                    lat_start(nxt)
            pace(place, nxt)
            lon_copy(0, nxt, c).start()
            lon_copy(1, nxt, c).start()

    for i in columns[:2]:
        column_in[i].wait()
        load_column(i)
    for c in ORDER:
        pack_east(0, c, [tile(0, cx - 1, c * CHUNK, k) for k in range(TILES)])
        pack_west(0, c, [tile(0, 0, c * CHUNK, k) for k in range(TILES)])
    peers = 2 + jnp.minimum(lat, 1) + jnp.minimum(n_lat - 1 - lat, 1)
    pl.semaphore_wait(barrier, peers)

    def rest_of_start():
        for i in columns[2:]:
            column_in[i].wait()
            load_column(i)
        lat_start(0)
        zero = jnp.zeros((8, WIDE), jnp.float32)

        @pl.when(lat == 0)
        def _():
            for par in range(2):
                for i in range(cx):
                    field[par, i, 0:PAD, :] = zero

        @pl.when(lat == n_lat - 1)
        def _():
            for par in range(2):
                for i in range(cx):
                    field[par, i, PAD + cy : PAD + cy + PAD, :] = zero

    def rest_of_tables():
        couple_in.wait()
        couple[...] = jnp.zeros(couple.shape, couple.dtype)
        couple[0:bins, 0:bins] = couple_raw[...]

    for place, c in enumerate(ORDER):
        if place >= DEPTH:
            pace(place, 0)
        lon_copy(0, 0, c).start()
        lon_copy(1, 0, c).start()
        if place < 3:
            (rest_of_start, tables, rest_of_tables)[place]()

    def loop(n, carry):
        step_body(n, False)
        return carry

    lax.fori_loop(0, STEPS - 1, loop, 0)
    step_body(STEPS - 1, True)
    for par in range(2):
        lat_wait_send(par)
    for c in ORDER[len(ORDER) - DEPTH :]:
        lon_copy(0, (STEPS - 1) % 2, c).wait_send()
        lon_copy(1, (STEPS - 1) % 2, c).wait_send()


def on_device(n_lon, n_lat, spectrum, sea_mask, ice_flags, wind_forcing, group_speed, coupling):
    cx, cy, bins = spectrum.shape
    freqs = group_speed.shape[0]
    chunks = cy // CHUNK
    f32 = jnp.float32
    dma = pltpu.SemaphoreType.DMA
    scratch = [
        pltpu.VMEM((cx, cy, bins), f32),
        pltpu.VMEM((2, cx, cy + 2 * PAD, WIDE), f32),
        pltpu.VMEM((cx, cy), jnp.int32),
        pltpu.VMEM((cx, cy), jnp.int32),
        pltpu.VMEM((cx, cy), f32),
        pltpu.SMEM((freqs,), f32),
        pltpu.VMEM((bins, bins), jnp.bfloat16),
        pltpu.VMEM((WIDE, WIDE), jnp.bfloat16),
        pltpu.VMEM((8, WIDE), f32),
        pltpu.VMEM((cy, WIDE), f32),
        pltpu.VMEM((cy, WIDE), f32),
        pltpu.VMEM((8, WIDE), f32),
        pltpu.VMEM((cx, cy, LANES), f32),
        pltpu.VMEM((cx, cy, LANES), f32),
        pltpu.VMEM((2 * (cx - 2) * CHUNK, WIDE), f32),
        pltpu.VMEM((2 * (cx - 2) * CHUNK, WIDE), jnp.bfloat16),
        pltpu.VMEM((2, 2, chunks, WIRE, LANES), f32),
        pltpu.VMEM((2, 2, chunks, WIRE, LANES), f32),
        dma((cx + 6,)),
        dma((2, 2, chunks)),
        dma((2, 2, chunks)),
        dma((2, 2)),
        dma((2, 2)),
    ]
    anywhere = pl.BlockSpec(memory_space=pl.ANY)
    return pl.pallas_call(
        functools.partial(kernel, (n_lon, n_lat, bins, freqs)),
        out_shape=pltpu.VMEM((cx, cy, bins), f32),
        in_specs=[anywhere] * 7,
        out_specs=pl.BlockSpec(memory_space=pltpu.VMEM),
        scratch_shapes=scratch,
        compiler_params=pltpu.CompilerParams(
            collective_id=0, has_side_effects=True, vmem_limit_bytes=63000 * 1024
        ),
    )(spectrum, sea_mask, ice_flags, wind_forcing, group_speed, coupling, jnp.asarray(direction_rows(freqs)))


def solution(mesh):
    placed = (P("lon", "lat", None), P("lon", "lat"), P("lon", "lat"), P("lon", "lat"), P(), P())
    return jax.shard_map(
        functools.partial(on_device, mesh.shape["lon"], mesh.shape["lat"]),
        mesh=mesh, in_specs=placed, out_specs=P("lon", "lat", None), check_vma=False,
    )
```

```python
import functools
import math

import jax
import jax.numpy as jnp
import numpy as np
from jax import lax
from jax.experimental import pallas as pl
from jax.experimental.pallas import tpu as pltpu
from jax.sharding import PartitionSpec as P

DIRS = 36
STEPS = 4
TIME_STEP = 0.2
DISSIPATION = 0.5
LANES = 128
TILES = 6
WIDE = TILES * LANES
CHUNK = 16
BLOCK = 16
WIRE = 2 * CHUNK + CHUNK // 2 + 1
DEPTH = 2
PAD = 8
ORDER = (0, 3, 1, 2)
MESH = pl.DeviceIdType.MESH


def direction_rows(freqs):
    theta = ((np.arange(DIRS, dtype=np.float32) + np.float32(0.5)) * np.float32(2.0 * math.pi / DIRS))
    rows = np.zeros((8, WIDE), np.float32)
    bins = DIRS * freqs
    rows[0, :bins] = np.repeat(np.abs(np.cos(theta)), freqs)
    rows[1, :bins] = np.repeat(np.abs(np.sin(theta)), freqs)
    rows[2, :bins] = np.tile(np.arange(freqs), DIRS)
    rows[2, bins:] = -1.0
    return rows


def kernel(
    sizes,
    spectrum, sea, ice, wind, speed, coupling, rows_in,
    out,
    raw, field, sea_v, ice_v, wind_v, speed_s, couple_raw, couple, rows_v,
    keep, along_x, along_y, share, gain, moved, rounded,
    send, recv,
    in_sem, lon_send, lon_recv, lat_send, lat_recv,
):
    n_lon, n_lat, bins, freqs = sizes
    cx, cy = spectrum.shape[0], spectrum.shape[1]
    chunks = cy // CHUNK
    lon, lat = lax.axis_index("lon"), lax.axis_index("lat")
    east, west = lax.rem(lon + 1, n_lon), lax.rem(lon + n_lon - 1, n_lon)
    has_south, has_north = lat > 0, lat < n_lat - 1
    lane = lax.broadcasted_iota(jnp.int32, (CHUNK, LANES), 1)
    sub = lax.broadcasted_iota(jnp.int32, (8, LANES), 0)
    lane8 = lane[0:8]
    free_lanes = ((lane8 >= 38) & (lane8 < 102), (lane8 < 34) | (lane8 >= 98))
    lane_block = lax.broadcasted_iota(jnp.int32, (BLOCK, LANES), 1)

    barrier = pltpu.get_barrier_semaphore()
    pl.semaphore_signal(barrier, inc=1, device_id={"lon": east}, device_id_type=MESH)
    pl.semaphore_signal(barrier, inc=1, device_id={"lon": west}, device_id_type=MESH)

    @pl.when(has_south)
    def _():
        pl.semaphore_signal(barrier, inc=1, device_id={"lat": lat - 1}, device_id_type=MESH)

    @pl.when(has_north)
    def _():
        pl.semaphore_signal(barrier, inc=1, device_id={"lat": lat + 1}, device_id_type=MESH)

    columns = (0, cx - 1) + tuple(range(1, cx - 1))
    column_in = {i: pltpu.make_async_copy(spectrum.at[i], raw.at[i], in_sem.at[i]) for i in columns}
    sea_in, *small = [
        pltpu.make_async_copy(src, dst, in_sem.at[cx + n])
        for n, (src, dst) in enumerate(
            [(sea, sea_v), (ice, ice_v), (wind, wind_v), (speed, speed_s), (rows_in, rows_v)]
        )
    ]
    couple_in = pltpu.make_async_copy(coupling, couple_raw, in_sem.at[cx + 5])
    sea_in.start()
    for i in columns[:2]:
        column_in[i].start()
    for copy in small:
        copy.start()
    for i in columns[2:]:
        column_in[i].start()
    couple_in.start()

    sea_in.wait()
    sea_f = sea_v[...].astype(jnp.float32)
    sea_t = jnp.transpose(sea_f)

    def load_column(i):
        sea_i = jnp.broadcast_to(sea_t[:, i : i + 1], (cy, LANES))
        for k in range(TILES):
            cut = slice(k * LANES, (k + 1) * LANES)
            if (k + 1) * LANES <= bins:
                field[0, i, PAD : PAD + cy, cut] = raw[i, :, cut] * sea_i
            else:
                tail = bins - k * LANES
                last = raw[i, :, k * LANES : bins] * sea_i[:, :tail]
                field[0, i, PAD : PAD + cy, cut] = jnp.concatenate(
                    [last, jnp.zeros((cy, LANES - tail), jnp.float32)], axis=1
                )

    def lon_copy(side, par, c):
        return pltpu.make_async_remote_copy(
            src_ref=send.at[side, par, c],
            dst_ref=recv.at[side, par, c],
            send_sem=lon_send.at[side, par, c],
            recv_sem=lon_recv.at[side, par, c],
            device_id={"lon": west if side else east},
            device_id_type=MESH,
        )

    def lat_copy(side, par):
        if side == 0:
            src = field.at[par, :, PAD + cy - 1 : PAD + cy, 0 : 3 * LANES]
            dst = field.at[par, :, PAD - 1 : PAD, 0 : 3 * LANES]
        else:
            src = field.at[par, :, PAD : PAD + 1, 2 * LANES : WIDE]
            dst = field.at[par, :, PAD + cy : PAD + cy + 1, 2 * LANES : WIDE]
        return pltpu.make_async_remote_copy(
            src_ref=src,
            dst_ref=dst,
            send_sem=lat_send.at[side, par],
            recv_sem=lat_recv.at[side, par],
            device_id={"lat": lat - 1 if side else lat + 1},
            device_id_type=MESH,
        )

    def lat_start(par):
        @pl.when(has_north)
        def _():
            lat_copy(0, par).start()

        @pl.when(has_south)
        def _():
            lat_copy(1, par).start()

    def lat_wait_send(par):
        @pl.when(has_north)
        def _():
            lat_copy(0, par).wait_send()

        @pl.when(has_south)
        def _():
            lat_copy(1, par).wait_send()

    def lat_wait_recv(par):
        @pl.when(has_south)
        def _():
            lat_copy(0, par).wait_recv()

        @pl.when(has_north)
        def _():
            lat_copy(1, par).wait_recv()

    def tables():
        for copy in small:
            copy.wait()
        speed_row = jnp.zeros((1, WIDE), jnp.float32)
        which = rows_v[2:3, :]
        for f in range(freqs):
            speed_row = jnp.where(which == f, speed_s[f], speed_row)
        scaled_x = 0.225 * (rows_v[0:1, :] * speed_row)
        scaled_y = 0.45 * (rows_v[1:2, :] * speed_row)
        row = (lat * cy + lax.broadcasted_iota(jnp.int32, (cy, LANES), 0)).astype(jnp.float32)
        phi = (-60.0 + 120.0 * (row + 0.5) / (cy * n_lat)) * (math.pi / 180.0)
        square = phi * phi
        cosine = jnp.full((cy, LANES), 1.0 / math.factorial(16), jnp.float32)
        for term in range(7, -1, -1):
            cosine = cosine * square + (-1.0) ** term / math.factorial(2 * term)
        inverse = 1.0 / cosine
        along_y[...] = jnp.broadcast_to(scaled_y, (8, WIDE))
        for k in range(TILES):
            cut = slice(k * LANES, (k + 1) * LANES)
            speed_x = inverse * scaled_x[:, cut]
            along_x[:, cut] = speed_x
            keep[:, cut] = 1.0 - speed_x - scaled_y[:, cut]

        forcing = wind_v[...] * (1.0 - ice_v[...].astype(jnp.float32))
        gain_t = jnp.transpose(sea_f * (1.0 + TIME_STEP * forcing))
        for i in range(cx):
            share[i] = TIME_STEP * jnp.broadcast_to(sea_t[:, i : i + 1], (cy, LANES))
            gain[i] = jnp.broadcast_to(gain_t[:, i : i + 1], (cy, LANES))

    def fold(side, par, c, first, second, near, far, left, at):
        send[side, par, c, 0:16] = first
        send[side, par, c, 16:32] = second
        send[side, par, c, 32:40] = jnp.where(free_lanes[side], far, near)
        line = None
        for half in range(2):
            body = left[8 * half : 8 * half + 8]
            rows = [pltpu.roll(body, (32 * half + 4 * r - at) % LANES, 1) for r in range(8)]
            for r in range(8):
                spot = 32 * half + 4 * r
                pick = (sub == r) & (lane8 >= spot) & (lane8 < spot + 4)
                line = jnp.where(pick, rows[r], 0.0 if line is None else line)
        send[side, par, c, 40:41] = jnp.sum(line, axis=0, keepdims=True)

    def unfold(side, par, c, at):
        body = recv[side, par, c, 32:40]
        line = jnp.broadcast_to(recv[side, par, c, 40:41], (8, LANES))
        rest, left = jnp.concatenate([body, pltpu.roll(body, 64, 1)], axis=0), []
        for half in range(2):
            rows = [pltpu.roll(line, (at - 32 * half - 4 * r) % LANES, 1) for r in range(8)]
            tail = rows[0]
            for r in range(1, 8):
                tail = jnp.where(sub == r, rows[r], tail)
            left.append(tail)
        return recv[side, par, c, 0:16], recv[side, par, c, 16:32], rest, jnp.concatenate(left, axis=0)

    def pack_east(par, c, t):
        low, high = slice(0, 8), slice(8, 16)
        near = jnp.where(lane8 < 34, t[1][low], jnp.where(lane8 < 38, pltpu.roll(t[5][low], 34, 1), t[3][low]))
        mixed = jnp.where(lane8 < 34, t[1][high], t[3][high])
        far = jnp.where((lane8 >= 98) & (lane8 < 102), pltpu.roll(t[5][high], 98, 1), pltpu.roll(mixed, 64, 1))
        fold(0, par, c, t[0], t[4], near, far, t[5], 4)

    def pack_west(par, c, t):
        second = jnp.where(lane < 34, t[3], t[1])
        fold(1, par, c, t[2], second, t[3][0:8], pltpu.roll(t[3][8:16], 64, 1), t[3], 98)

    def unpack_east(par, c):
        first, second, rest, left = unfold(0, par, c, 4)
        body = recv[0, par, c, 32:40]
        four = jnp.concatenate([pltpu.roll(body, LANES - 34, 1), pltpu.roll(body, LANES - 98, 1)], axis=0)
        return {0: first, 1: rest, 3: rest, 4: second, 5: jnp.where(lane < 4, four, left)}

    def unpack_west(par, c):
        first, second, rest, left = unfold(1, par, c, 98)
        return {1: second, 2: first, 3: jnp.where(lane < 34, second, jnp.where(lane < 98, rest, left))}

    def tile(par, i, r0, rows, k):
        return field[par, i, PAD + r0 : PAD + r0 + rows, k * LANES : (k + 1) * LANES]

    def advect(par, i, r0, rows):
        at = lane if rows == CHUNK else lane_block
        if i == 0:
            from_west = unpack_east(par, r0 // CHUNK)
        else:
            from_west = {k: tile(par, i - 1, r0, rows, k) for k in (0, 1, 3, 4, 5)}
        if i == cx - 1:
            from_east = unpack_west(par, r0 // CHUNK)
        else:
            from_east = {k: tile(par, i + 1, r0, rows, k) for k in (1, 2, 3)}
        up_x = [
            from_west[0],
            jnp.where(at < 34, from_west[1], from_east[1]),
            from_east[2],
            jnp.where(at < 102, from_east[3], from_west[3]),
            from_west[4],
            from_west[5],
        ]
        out_tiles = []
        for k in range(TILES):
            span = slice(r0, r0 + rows)
            cut = slice(k * LANES, (k + 1) * LANES)
            south = tile(par, i, r0 - 1, rows, k) if k <= 2 else None
            north = tile(par, i, r0 + 1, rows, k) if k >= 2 else None
            up_y = south if north is None else north if south is None else jnp.where(at < 68, south, north)
            speed_y = jnp.concatenate([along_y[:, cut]] * (rows // 8), axis=0)
            out_tiles.append(
                tile(par, i, r0, rows, k) * keep[span, cut] + along_x[span, cut] * up_x[k] + speed_y * up_y
            )
        return out_tiles

    def cell_gain(i, r0, rows, t):
        span = slice(r0, r0 + rows)
        total = jnp.sum((t[0] + t[1]) + (t[2] + t[3]) + (t[4] + t[5]), axis=1, keepdims=True)
        return gain[i, span, :] - share[i, span, :] * (total * (DISSIPATION / bins))

    def put(par, i, r0, rows, tiles, last):
        for k in range(TILES):
            if not last:
                field[par, i, PAD + r0 : PAD + r0 + rows, k * LANES : (k + 1) * LANES] = tiles[k]
            elif (k + 1) * LANES <= bins:
                out[i, r0 : r0 + rows, k * LANES : (k + 1) * LANES] = tiles[k]
            else:
                out[i, r0 : r0 + rows, k * LANES : bins] = tiles[k][:, : bins - k * LANES]

    def edges(par, c, last):
        r0 = c * CHUNK
        both = [advect(par, i, r0, CHUNK) for i in (0, cx - 1)]
        gains = [cell_gain(i, r0, CHUNK, t) for i, t in zip((0, cx - 1), both)]
        for k in range(TILES):
            pair = jnp.concatenate([both[0][k], both[1][k]], axis=0)
            rounded[0 : 2 * CHUNK, k * LANES : (k + 1) * LANES] = pair.astype(jnp.bfloat16)
        transfer = jnp.dot(rounded[0 : 2 * CHUNK, :], couple[...], preferred_element_type=jnp.float32)
        results = []
        for n, i in enumerate((0, cx - 1)):
            part = share[i, r0 : r0 + CHUNK, :]
            lines = slice(n * CHUNK, (n + 1) * CHUNK)
            tiles = [
                both[n][k] * gains[n] + transfer[lines, k * LANES : (k + 1) * LANES] * part for k in range(TILES)
            ]
            put(1 - par, i, r0, CHUNK, tiles, last)
            results.append(tiles)
        return results

    def inside(par, blocks, last):
        spots = [(i, b * BLOCK) for b in blocks for i in range(1, cx - 1)]
        gains = []
        for n, (i, r0) in enumerate(spots):
            t = advect(par, i, r0, BLOCK)
            gains.append(cell_gain(i, r0, BLOCK, t))
            for k in range(TILES):
                cut = slice(k * LANES, (k + 1) * LANES)
                moved[n * BLOCK : (n + 1) * BLOCK, cut] = t[k]
                rounded[n * BLOCK : (n + 1) * BLOCK, cut] = t[k].astype(jnp.bfloat16)
        height = len(spots) * BLOCK
        transfer = jnp.dot(rounded[0:height, :], couple[...], preferred_element_type=jnp.float32)
        for n, (i, r0) in enumerate(spots):
            part = share[i, r0 : r0 + BLOCK, :]
            tiles = []
            for k in range(TILES):
                cut = slice(k * LANES, (k + 1) * LANES)
                lines = slice(n * BLOCK, (n + 1) * BLOCK)
                tiles.append(moved[lines, cut] * gains[n] + transfer[lines, cut] * part)
            put(1 - par, i, r0, BLOCK, tiles, last)

    def pace(place, par):
        back = place - DEPTH
        which = par if back >= 0 else 1 - par
        for side in range(2):
            lon_copy(side, which, ORDER[back]).wait_send()

    def step_body(n, last):
        par = lax.rem(n, 2)
        nxt = 1 - par
        if not last:
            @pl.when(n >= 1)
            def _():
                lat_wait_send(nxt)

        lat_wait_recv(par)
        inside(par, (0, 3), last)
        if last:
            inside(par, (1, 2), last)
        for place, c in enumerate(ORDER):
            lon_copy(0, par, c).wait_recv()
            lon_copy(1, par, c).wait_recv()
            first, final = edges(par, c, last)
            if last:
                continue
            pack_east(nxt, c, final)
            pack_west(nxt, c, first)
            pace(place, nxt)
            lon_copy(0, nxt, c).start()
            lon_copy(1, nxt, c).start()
            if place == 1:
                lat_start(nxt)
        if not last:
            inside(par, (1, 2), last)

    for i in columns[:2]:
        column_in[i].wait()
        load_column(i)
    for c in ORDER:
        pack_east(0, c, [tile(0, cx - 1, c * CHUNK, CHUNK, k) for k in range(TILES)])
        pack_west(0, c, [tile(0, 0, c * CHUNK, CHUNK, k) for k in range(TILES)])
    peers = 2 + jnp.minimum(lat, 1) + jnp.minimum(n_lat - 1 - lat, 1)
    pl.semaphore_wait(barrier, peers)

    def rest_of_start():
        for i in columns[2:]:
            column_in[i].wait()
            load_column(i)
        lat_start(0)
        zero = jnp.zeros((8, WIDE), jnp.float32)

        @pl.when(lat == 0)
        def _():
            for par in range(2):
                for i in range(cx):
                    field[par, i, 0:PAD, :] = zero

        @pl.when(lat == n_lat - 1)
        def _():
            for par in range(2):
                for i in range(cx):
                    field[par, i, PAD + cy : PAD + cy + PAD, :] = zero

    def rest_of_tables():
        couple_in.wait()
        couple[...] = jnp.zeros(couple.shape, couple.dtype)
        couple[0:bins, 0:bins] = couple_raw[...]

    for place, c in enumerate(ORDER):
        if place >= DEPTH:
            pace(place, 0)
        lon_copy(0, 0, c).start()
        lon_copy(1, 0, c).start()
        if DEPTH - 1 <= place < DEPTH + 2:
            (rest_of_start, tables, rest_of_tables)[place - DEPTH + 1]()

    def loop(n, carry):
        step_body(n, False)
        return carry

    lax.fori_loop(0, STEPS - 1, loop, 0)
    step_body(STEPS - 1, True)
    for par in range(2):
        lat_wait_send(par)
    for c in ORDER[len(ORDER) - DEPTH :]:
        lon_copy(0, (STEPS - 1) % 2, c).wait_send()
        lon_copy(1, (STEPS - 1) % 2, c).wait_send()


def on_device(n_lon, n_lat, spectrum, sea_mask, ice_flags, wind_forcing, group_speed, coupling):
    cx, cy, bins = spectrum.shape
    freqs = group_speed.shape[0]
    chunks = cy // CHUNK
    f32 = jnp.float32
    dma = pltpu.SemaphoreType.DMA
    scratch = [
        pltpu.VMEM((cx, cy, bins), f32),
        pltpu.VMEM((2, cx, cy + 2 * PAD, WIDE), f32),
        pltpu.VMEM((cx, cy), jnp.int32),
        pltpu.VMEM((cx, cy), jnp.int32),
        pltpu.VMEM((cx, cy), f32),
        pltpu.SMEM((freqs,), f32),
        pltpu.VMEM((bins, bins), jnp.bfloat16),
        pltpu.VMEM((WIDE, WIDE), jnp.bfloat16),
        pltpu.VMEM((8, WIDE), f32),
        pltpu.VMEM((cy, WIDE), f32),
        pltpu.VMEM((cy, WIDE), f32),
        pltpu.VMEM((8, WIDE), f32),
        pltpu.VMEM((cx, cy, LANES), f32),
        pltpu.VMEM((cx, cy, LANES), f32),
        pltpu.VMEM((2 * (cx - 2) * BLOCK, WIDE), f32),
        pltpu.VMEM((2 * (cx - 2) * BLOCK, WIDE), jnp.bfloat16),
        pltpu.VMEM((2, 2, chunks, WIRE, LANES), f32),
        pltpu.VMEM((2, 2, chunks, WIRE, LANES), f32),
        dma((cx + 6,)),
        dma((2, 2, chunks)),
        dma((2, 2, chunks)),
        dma((2, 2)),
        dma((2, 2)),
    ]
    anywhere = pl.BlockSpec(memory_space=pl.ANY)
    return pl.pallas_call(
        functools.partial(kernel, (n_lon, n_lat, bins, freqs)),
        out_shape=pltpu.VMEM((cx, cy, bins), f32),
        in_specs=[anywhere] * 7,
        out_specs=pl.BlockSpec(memory_space=pltpu.VMEM),
        scratch_shapes=scratch,
        compiler_params=pltpu.CompilerParams(
            collective_id=0, has_side_effects=True, vmem_limit_bytes=63000 * 1024
        ),
    )(spectrum, sea_mask, ice_flags, wind_forcing, group_speed, coupling, jnp.asarray(direction_rows(freqs)))


def solution(mesh):
    placed = (P("lon", "lat", None), P("lon", "lat"), P("lon", "lat"), P("lon", "lat"), P(), P())
    return jax.shard_map(
        functools.partial(on_device, mesh.shape["lon"], mesh.shape["lat"]),
        mesh=mesh, in_specs=placed, out_specs=P("lon", "lat", None), check_vma=False,
    )
```

```python
import functools
import math

import jax
import jax.numpy as jnp
import numpy as np
from jax import lax
from jax.experimental import pallas as pl
from jax.experimental.pallas import tpu as pltpu
from jax.sharding import PartitionSpec as P

DIRS = 36
STEPS = 4
TIME_STEP = 0.2
DISSIPATION = 0.5
LANES = 128
TILES = 6
WIDE = TILES * LANES
CHUNK = 16
BLOCK = 16
WIRE = 2 * CHUNK + CHUNK // 2 + 1
DEPTH = 2
PAD = 8
ORDER = (0, 3, 1, 2)
MESH = pl.DeviceIdType.MESH


def direction_rows(freqs):
    theta = ((np.arange(DIRS, dtype=np.float32) + np.float32(0.5)) * np.float32(2.0 * math.pi / DIRS))
    rows = np.zeros((8, WIDE), np.float32)
    bins = DIRS * freqs
    rows[0, :bins] = np.repeat(np.abs(np.cos(theta)), freqs)
    rows[1, :bins] = np.repeat(np.abs(np.sin(theta)), freqs)
    rows[2, :bins] = np.tile(np.arange(freqs), DIRS)
    rows[2, bins:] = -1.0
    return rows


def kernel(
    sizes,
    spectrum, sea, ice, wind, speed, coupling, rows_in,
    out,
    raw, field, sea_v, ice_v, wind_v, speed_s, couple_raw, couple, rows_v,
    keep, along_x, along_y, share, gain, moved, rounded,
    send, recv,
    in_sem, lon_send, lon_recv, lat_send, lat_recv,
):
    n_lon, n_lat, bins, freqs = sizes
    cx, cy = spectrum.shape[0], spectrum.shape[1]
    chunks = cy // CHUNK
    lon, lat = lax.axis_index("lon"), lax.axis_index("lat")
    east, west = lax.rem(lon + 1, n_lon), lax.rem(lon + n_lon - 1, n_lon)
    has_south, has_north = lat > 0, lat < n_lat - 1
    lane = lax.broadcasted_iota(jnp.int32, (CHUNK, LANES), 1)
    sub = lax.broadcasted_iota(jnp.int32, (8, LANES), 0)
    lane8 = lane[0:8]
    free_lanes = ((lane8 >= 38) & (lane8 < 102), (lane8 < 34) | (lane8 >= 98))
    lane_block = lax.broadcasted_iota(jnp.int32, (BLOCK, LANES), 1)

    barrier = pltpu.get_barrier_semaphore()
    pl.semaphore_signal(barrier, inc=1, device_id={"lon": east}, device_id_type=MESH)
    pl.semaphore_signal(barrier, inc=1, device_id={"lon": west}, device_id_type=MESH)

    @pl.when(has_south)
    def _():
        pl.semaphore_signal(barrier, inc=1, device_id={"lat": lat - 1}, device_id_type=MESH)

    @pl.when(has_north)
    def _():
        pl.semaphore_signal(barrier, inc=1, device_id={"lat": lat + 1}, device_id_type=MESH)

    columns = (0, cx - 1) + tuple(range(1, cx - 1))
    column_in = {i: pltpu.make_async_copy(spectrum.at[i], raw.at[i], in_sem.at[i]) for i in columns}
    sea_in, *small = [
        pltpu.make_async_copy(src, dst, in_sem.at[cx + n])
        for n, (src, dst) in enumerate(
            [(sea, sea_v), (ice, ice_v), (wind, wind_v), (speed, speed_s), (rows_in, rows_v)]
        )
    ]
    couple_in = pltpu.make_async_copy(coupling, couple_raw, in_sem.at[cx + 5])
    sea_in.start()
    for i in columns[:2]:
        column_in[i].start()
    for copy in small:
        copy.start()
    for i in columns[2:]:
        column_in[i].start()
    couple_in.start()

    sea_in.wait()
    sea_f = sea_v[...].astype(jnp.float32)
    sea_t = jnp.transpose(sea_f)

    def load_column(i):
        sea_i = jnp.broadcast_to(sea_t[:, i : i + 1], (cy, LANES))
        for k in range(TILES):
            cut = slice(k * LANES, (k + 1) * LANES)
            if (k + 1) * LANES <= bins:
                field[0, i, PAD : PAD + cy, cut] = raw[i, :, cut] * sea_i
            else:
                tail = bins - k * LANES
                last = raw[i, :, k * LANES : bins] * sea_i[:, :tail]
                field[0, i, PAD : PAD + cy, cut] = jnp.concatenate(
                    [last, jnp.zeros((cy, LANES - tail), jnp.float32)], axis=1
                )

    def lon_copy(side, par, c):
        return pltpu.make_async_remote_copy(
            src_ref=send.at[side, par, c, 0:WIRE],
            dst_ref=recv.at[side, par, c, 0:WIRE],
            send_sem=lon_send.at[side, par, c],
            recv_sem=lon_recv.at[side, par, c],
            device_id={"lon": west if side else east},
            device_id_type=MESH,
        )

    def lat_copy(side, par):
        if side == 0:
            src = field.at[par, :, PAD + cy - 1 : PAD + cy, 0 : 3 * LANES]
            dst = field.at[par, :, PAD - 1 : PAD, 0 : 3 * LANES]
        else:
            src = field.at[par, :, PAD : PAD + 1, 2 * LANES : WIDE]
            dst = field.at[par, :, PAD + cy : PAD + cy + 1, 2 * LANES : WIDE]
        return pltpu.make_async_remote_copy(
            src_ref=src,
            dst_ref=dst,
            send_sem=lat_send.at[side, par],
            recv_sem=lat_recv.at[side, par],
            device_id={"lat": lat - 1 if side else lat + 1},
            device_id_type=MESH,
        )

    def lat_start(par):
        @pl.when(has_north)
        def _():
            lat_copy(0, par).start()

        @pl.when(has_south)
        def _():
            lat_copy(1, par).start()

    def lat_wait_send(par):
        @pl.when(has_north)
        def _():
            lat_copy(0, par).wait_send()

        @pl.when(has_south)
        def _():
            lat_copy(1, par).wait_send()

    def lat_wait_recv(par):
        @pl.when(has_south)
        def _():
            lat_copy(0, par).wait_recv()

        @pl.when(has_north)
        def _():
            lat_copy(1, par).wait_recv()

    def tables():
        for copy in small:
            copy.wait()
        speed_row = jnp.zeros((1, WIDE), jnp.float32)
        which = rows_v[2:3, :]
        for f in range(freqs):
            speed_row = jnp.where(which == f, speed_s[f], speed_row)
        scaled_x = 0.225 * (rows_v[0:1, :] * speed_row)
        scaled_y = 0.45 * (rows_v[1:2, :] * speed_row)
        row = (lat * cy + lax.broadcasted_iota(jnp.int32, (cy, LANES), 0)).astype(jnp.float32)
        phi = (-60.0 + 120.0 * (row + 0.5) / (cy * n_lat)) * (math.pi / 180.0)
        square = phi * phi
        cosine = jnp.full((cy, LANES), 1.0 / math.factorial(16), jnp.float32)
        for term in range(7, -1, -1):
            cosine = cosine * square + (-1.0) ** term / math.factorial(2 * term)
        inverse = 1.0 / cosine
        along_y[...] = jnp.broadcast_to(scaled_y, (8, WIDE))
        for k in range(TILES):
            cut = slice(k * LANES, (k + 1) * LANES)
            speed_x = inverse * scaled_x[:, cut]
            along_x[:, cut] = speed_x
            keep[:, cut] = 1.0 - speed_x - scaled_y[:, cut]

        forcing = wind_v[...] * (1.0 - ice_v[...].astype(jnp.float32))
        gain_t = jnp.transpose(sea_f * (1.0 + TIME_STEP * forcing))
        for i in range(cx):
            share[i] = TIME_STEP * jnp.broadcast_to(sea_t[:, i : i + 1], (cy, LANES))
            gain[i] = jnp.broadcast_to(gain_t[:, i : i + 1], (cy, LANES))

    def fold(side, par, c, first, second, near, far, left, at):
        send[side, par, c, 0:16] = first
        send[side, par, c, 16:32] = second
        send[side, par, c, 32:40] = jnp.where(free_lanes[side], far, near)
        line = None
        for half in range(2):
            body = left[8 * half : 8 * half + 8]
            rows = [pltpu.roll(body, (32 * half + 4 * r - at) % LANES, 1) for r in range(8)]
            for r in range(8):
                spot = 32 * half + 4 * r
                pick = (sub == r) & (lane8 >= spot) & (lane8 < spot + 4)
                line = jnp.where(pick, rows[r], 0.0 if line is None else line)
        send[side, par, c, 40:41] = jnp.sum(line, axis=0, keepdims=True)

    def unfold(side, par, c, at):
        body = recv[side, par, c, 32:40]
        line = jnp.broadcast_to(recv[side, par, c, 40:41], (8, LANES))
        rest, left = jnp.concatenate([body, pltpu.roll(body, 64, 1)], axis=0), []
        for half in range(2):
            rows = [pltpu.roll(line, (at - 32 * half - 4 * r) % LANES, 1) for r in range(8)]
            tail = rows[0]
            for r in range(1, 8):
                tail = jnp.where(sub == r, rows[r], tail)
            left.append(tail)
        return recv[side, par, c, 0:16], recv[side, par, c, 16:32], rest, jnp.concatenate(left, axis=0)

    def pack_east(par, c, t):
        low, high = slice(0, 8), slice(8, 16)
        near = jnp.where(lane8 < 34, t[1][low], jnp.where(lane8 < 38, pltpu.roll(t[5][low], 34, 1), t[3][low]))
        mixed = jnp.where(lane8 < 34, t[1][high], t[3][high])
        far = jnp.where((lane8 >= 98) & (lane8 < 102), pltpu.roll(t[5][high], 98, 1), pltpu.roll(mixed, 64, 1))
        fold(0, par, c, t[0], t[4], near, far, t[5], 4)

    def pack_west(par, c, t):
        second = jnp.where(lane < 34, t[3], t[1])
        fold(1, par, c, t[2], second, t[3][0:8], pltpu.roll(t[3][8:16], 64, 1), t[3], 98)

    def unpack_east(par, c):
        first, second, rest, left = unfold(0, par, c, 4)
        body = recv[0, par, c, 32:40]
        four = jnp.concatenate([pltpu.roll(body, LANES - 34, 1), pltpu.roll(body, LANES - 98, 1)], axis=0)
        return {0: first, 1: rest, 3: rest, 4: second, 5: jnp.where(lane < 4, four, left)}

    def unpack_west(par, c):
        first, second, rest, left = unfold(1, par, c, 98)
        return {1: second, 2: first, 3: jnp.where(lane < 34, second, jnp.where(lane < 98, rest, left))}

    def tile(par, i, r0, rows, k):
        return field[par, i, PAD + r0 : PAD + r0 + rows, k * LANES : (k + 1) * LANES]

    def advect(par, i, r0, rows):
        at = lane if rows == CHUNK else lane_block
        if i == 0:
            from_west = unpack_east(par, r0 // CHUNK)
        else:
            from_west = {k: tile(par, i - 1, r0, rows, k) for k in (0, 1, 3, 4, 5)}
        if i == cx - 1:
            from_east = unpack_west(par, r0 // CHUNK)
        else:
            from_east = {k: tile(par, i + 1, r0, rows, k) for k in (1, 2, 3)}
        up_x = [
            from_west[0],
            jnp.where(at < 34, from_west[1], from_east[1]),
            from_east[2],
            jnp.where(at < 102, from_east[3], from_west[3]),
            from_west[4],
            from_west[5],
        ]
        out_tiles = []
        for k in range(TILES):
            span = slice(r0, r0 + rows)
            cut = slice(k * LANES, (k + 1) * LANES)
            south = tile(par, i, r0 - 1, rows, k) if k <= 2 else None
            north = tile(par, i, r0 + 1, rows, k) if k >= 2 else None
            up_y = south if north is None else north if south is None else jnp.where(at < 68, south, north)
            speed_y = jnp.concatenate([along_y[:, cut]] * (rows // 8), axis=0)
            out_tiles.append(
                tile(par, i, r0, rows, k) * keep[span, cut] + along_x[span, cut] * up_x[k] + speed_y * up_y
            )
        return out_tiles

    def cell_gain(i, r0, rows, t):
        span = slice(r0, r0 + rows)
        total = jnp.sum((t[0] + t[1]) + (t[2] + t[3]) + (t[4] + t[5]), axis=1, keepdims=True)
        return gain[i, span, :] - share[i, span, :] * (total * (DISSIPATION / bins))

    def put(par, i, r0, rows, tiles, last):
        for k in range(TILES):
            if not last:
                field[par, i, PAD + r0 : PAD + r0 + rows, k * LANES : (k + 1) * LANES] = tiles[k]
            elif (k + 1) * LANES <= bins:
                out[i, r0 : r0 + rows, k * LANES : (k + 1) * LANES] = tiles[k]
            else:
                out[i, r0 : r0 + rows, k * LANES : bins] = tiles[k][:, : bins - k * LANES]

    def edges(par, c, last):
        r0 = c * CHUNK
        both = [advect(par, i, r0, CHUNK) for i in (0, cx - 1)]
        gains = [cell_gain(i, r0, CHUNK, t) for i, t in zip((0, cx - 1), both)]
        for k in range(TILES):
            pair = jnp.concatenate([both[0][k], both[1][k]], axis=0)
            rounded[0 : 2 * CHUNK, k * LANES : (k + 1) * LANES] = pair.astype(jnp.bfloat16)
        transfer = jnp.dot(rounded[0 : 2 * CHUNK, :], couple[...], preferred_element_type=jnp.float32)
        results = []
        for n, i in enumerate((0, cx - 1)):
            part = share[i, r0 : r0 + CHUNK, :]
            lines = slice(n * CHUNK, (n + 1) * CHUNK)
            tiles = [
                both[n][k] * gains[n] + transfer[lines, k * LANES : (k + 1) * LANES] * part for k in range(TILES)
            ]
            put(1 - par, i, r0, CHUNK, tiles, last)
            results.append(tiles)
        return results

    def inside(par, blocks, last):
        spots = [(i, b * BLOCK) for b in blocks for i in range(1, cx - 1)]
        gains = []
        for n, (i, r0) in enumerate(spots):
            t = advect(par, i, r0, BLOCK)
            gains.append(cell_gain(i, r0, BLOCK, t))
            for k in range(TILES):
                cut = slice(k * LANES, (k + 1) * LANES)
                moved[n * BLOCK : (n + 1) * BLOCK, cut] = t[k]
                rounded[n * BLOCK : (n + 1) * BLOCK, cut] = t[k].astype(jnp.bfloat16)
        height = len(spots) * BLOCK
        transfer = jnp.dot(rounded[0:height, :], couple[...], preferred_element_type=jnp.float32)
        for n, (i, r0) in enumerate(spots):
            part = share[i, r0 : r0 + BLOCK, :]
            tiles = []
            for k in range(TILES):
                cut = slice(k * LANES, (k + 1) * LANES)
                lines = slice(n * BLOCK, (n + 1) * BLOCK)
                tiles.append(moved[lines, cut] * gains[n] + transfer[lines, cut] * part)
            put(1 - par, i, r0, BLOCK, tiles, last)

    def pace(place, par):
        back = place - DEPTH
        which = par if back >= 0 else 1 - par
        for side in range(2):
            lon_copy(side, which, ORDER[back]).wait_send()

    def step_body(n, last):
        par = lax.rem(n, 2)
        nxt = 1 - par
        if not last:
            @pl.when(n >= 1)
            def _():
                lat_wait_send(nxt)

        lat_wait_recv(par)
        inside(par, (0, 3), last)
        if last:
            inside(par, (1, 2), last)
        for place, c in enumerate(ORDER):
            lon_copy(0, par, c).wait_recv()
            lon_copy(1, par, c).wait_recv()
            first, final = edges(par, c, last)
            if last:
                continue
            pack_east(nxt, c, final)
            pack_west(nxt, c, first)
            pace(place, nxt)
            lon_copy(0, nxt, c).start()
            lon_copy(1, nxt, c).start()
            if place == 1:
                lat_start(nxt)
        if not last:
            inside(par, (1, 2), last)

    for i in columns[:2]:
        column_in[i].wait()
        load_column(i)
    for c in ORDER:
        pack_east(0, c, [tile(0, cx - 1, c * CHUNK, CHUNK, k) for k in range(TILES)])
        pack_west(0, c, [tile(0, 0, c * CHUNK, CHUNK, k) for k in range(TILES)])
    peers = 2 + jnp.minimum(lat, 1) + jnp.minimum(n_lat - 1 - lat, 1)
    pl.semaphore_wait(barrier, peers)

    def rest_of_start():
        for i in columns[2:]:
            column_in[i].wait()
            load_column(i)
        lat_start(0)
        zero = jnp.zeros((8, WIDE), jnp.float32)

        @pl.when(lat == 0)
        def _():
            for par in range(2):
                for i in range(cx):
                    field[par, i, 0:PAD, :] = zero

        @pl.when(lat == n_lat - 1)
        def _():
            for par in range(2):
                for i in range(cx):
                    field[par, i, PAD + cy : PAD + cy + PAD, :] = zero

    def rest_of_tables():
        couple_in.wait()
        couple[...] = jnp.zeros(couple.shape, couple.dtype)
        couple[0:bins, 0:bins] = couple_raw[...]

    for place, c in enumerate(ORDER):
        if place >= DEPTH:
            pace(place, 0)
        lon_copy(0, 0, c).start()
        lon_copy(1, 0, c).start()
        if DEPTH - 1 <= place < DEPTH + 2:
            (rest_of_start, tables, rest_of_tables)[place - DEPTH + 1]()

    def loop(n, carry):
        step_body(n, False)
        return carry

    lax.fori_loop(0, STEPS - 1, loop, 0)
    step_body(STEPS - 1, True)
    for par in range(2):
        lat_wait_send(par)
    for c in ORDER[len(ORDER) - DEPTH :]:
        lon_copy(0, (STEPS - 1) % 2, c).wait_send()
        lon_copy(1, (STEPS - 1) % 2, c).wait_send()


def on_device(n_lon, n_lat, spectrum, sea_mask, ice_flags, wind_forcing, group_speed, coupling):
    cx, cy, bins = spectrum.shape
    freqs = group_speed.shape[0]
    chunks = cy // CHUNK
    f32 = jnp.float32
    dma = pltpu.SemaphoreType.DMA
    scratch = [
        pltpu.VMEM((cx, cy, bins), f32),
        pltpu.VMEM((2, cx, cy + 2 * PAD, WIDE), f32),
        pltpu.VMEM((cx, cy), jnp.int32),
        pltpu.VMEM((cx, cy), jnp.int32),
        pltpu.VMEM((cx, cy), f32),
        pltpu.SMEM((freqs,), f32),
        pltpu.VMEM((bins, bins), jnp.bfloat16),
        pltpu.VMEM((WIDE, WIDE), jnp.bfloat16),
        pltpu.VMEM((8, WIDE), f32),
        pltpu.VMEM((cy, WIDE), f32),
        pltpu.VMEM((cy, WIDE), f32),
        pltpu.VMEM((8, WIDE), f32),
        pltpu.VMEM((cx, cy, LANES), f32),
        pltpu.VMEM((cx, cy, LANES), f32),
        pltpu.VMEM((2 * (cx - 2) * BLOCK, WIDE), f32),
        pltpu.VMEM((2 * (cx - 2) * BLOCK, WIDE), jnp.bfloat16),
        pltpu.VMEM((2, 2, chunks, WIRE + 7, LANES), f32),
        pltpu.VMEM((2, 2, chunks, WIRE + 7, LANES), f32),
        dma((cx + 6,)),
        dma((2, 2, chunks)),
        dma((2, 2, chunks)),
        dma((2, 2)),
        dma((2, 2)),
    ]
    anywhere = pl.BlockSpec(memory_space=pl.ANY)
    return pl.pallas_call(
        functools.partial(kernel, (n_lon, n_lat, bins, freqs)),
        out_shape=pltpu.VMEM((cx, cy, bins), f32),
        in_specs=[anywhere] * 7,
        out_specs=pl.BlockSpec(memory_space=pltpu.VMEM),
        scratch_shapes=scratch,
        compiler_params=pltpu.CompilerParams(
            collective_id=0, has_side_effects=True, vmem_limit_bytes=63000 * 1024
        ),
    )(spectrum, sea_mask, ice_flags, wind_forcing, group_speed, coupling, jnp.asarray(direction_rows(freqs)))


def solution(mesh):
    placed = (P("lon", "lat", None), P("lon", "lat"), P("lon", "lat"), P("lon", "lat"), P(), P())
    return jax.shard_map(
        functools.partial(on_device, mesh.shape["lon"], mesh.shape["lat"]),
        mesh=mesh, in_specs=placed, out_specs=P("lon", "lat", None), check_vma=False,
    )
```
